1024 devices in a mesh: section: 128 (over z_hi, y, x, core), tensor: 8 (over z_lo).
Axes of the slice: x: 4, y: 8, z: 16 (z_hi: 2, z_lo: 8; z = z_hi * 8 + z_lo), core: 2. Of those that a mesh axis runs over, the one named last changes fastest.
Arguments:
- acts: bfloat16 [128, 2, 32, 4096], P('section', None, None, 'tensor'), may hold values from -6 to 6
- grads_in: bfloat16 [128, 2, 32, 4096], P('section', None, None, 'tensor'), may hold values from -6 to 6
- head_grads: bfloat16 [128, 2, 128, 1024], P('section', None, None, 'tensor'), may hold values from -6 to 6
- types: int32 [128, 2, 32], P('section'), may hold values 0 or 1
- gains: bfloat16 [128, 2, 2, 1024], P('section'), may hold values from 0.3984375 to 1.59375
- w_query: bfloat16 [128, 2, 4096, 1024], P('section', None, None, 'tensor'), may hold values from -0.09375 to 0.09375
- w_key: bfloat16 [128, 2, 4096, 128], P('section', None, None, 'tensor'), may hold values from -0.09375 to 0.09375
- w_value: bfloat16 [128, 2, 4096, 128], P('section', None, None, 'tensor'), may hold values from -0.09375 to 0.09375
Outputs:
- routed: bfloat16 [128, 2, 32, 4096], P('section', None, None, 'tensor')
The draws below stay inside these ranges and needn't reach their ends.
All inputs are finite; a program needn't handle non-finite values. No bound on the sum of `types` on one device may be relied on, other than what follows from the above.
Results may differ from the reference program's by a relative error of at most 0.0055.
Values may be sent and summed in bfloat16 or wider, within the bound.
No kernel may reach another device: no remote copies, remote signals or barrier semaphores. Data moves between devices by JAX's collectives and lax.ppermute only.
A program may use at most 64 MiB of HBM per device.

```python
import jax
import jax.numpy as jnp
from jax import lax

D = 4096
HEAD_DIM = 128
SUB = 4
SPANS = 2
TOK = 128
TOKQ = 32
N_SECTION = 128
N_TENSOR = 8


def set_ends(values, stream_key, smallest, top_value):
    longest = values.shape.index(max(values.shape))
    spots = []
    for shift in (0, 1):
        where = [jax.random.randint(jax.random.fold_in(stream_key, axis), (), 0, length) for axis, length in enumerate(values.shape)]
        where[longest] = (where[longest] + shift) % values.shape[longest]
        spots.append(tuple(where))
    return values.at[spots[0]].set(smallest).at[spots[1]].set(top_value)


def block_scale(own_key, shape, cuts, least, high):
    def one(dim, parts):
        steps = jax.random.uniform(jax.random.fold_in(jax.random.fold_in(own_key, 6), dim), (parts,), jnp.float32, least / len(cuts), high / len(cuts))
        return jnp.repeat(jnp.exp(steps), shape[dim] // parts).reshape((-1,) + (1,) * (len(shape) - dim - 1))

    gain = one(*cuts[0])
    for cut in cuts[1:]:
        gain = gain * one(*cut)
    return gain


def bell_draw(rng, dims, width, most, split=(), held_as=jnp.bfloat16):
    values = jax.random.normal(rng, dims, jnp.float32) * width
    if len(split) > 0:
        values = block_scale(rng, dims, split, -0.22, 0.18) * values
    return jnp.clip(values, min=-most, max=most).astype(held_as)


def setup_inputs(seed: int = 0) -> dict:
    keys = jax.random.split(jax.random.key(seed), 9)
    acts = bell_draw(keys[0], (N_SECTION, SPANS, TOKQ, D), 1.0, 6.0, ((0, 128), (3, 8)))
    grads_in = bell_draw(keys[1], (N_SECTION, SPANS, TOKQ, D), 1.0, 6.0, ((0, 128), (3, 8)))
    head_grads = bell_draw(keys[2], (N_SECTION, SPANS, TOK, HEAD_DIM * N_TENSOR), 1.0, 6.0, ((0, 128), (3, 8)))
    types = set_ends((jax.random.randint(keys[3], (N_SECTION, SPANS, TOKQ), 0, 2) < 1).astype(jnp.int32), jax.random.fold_in(keys[3], 1), 0, 1)
    gains = jnp.clip(1.0 + 0.12 * jax.random.normal(keys[4], (N_SECTION, SPANS, 2, D // SUB), jnp.float32), 0.3984375, 1.59375).astype(jnp.bfloat16)
    w_query = bell_draw(keys[5], (N_SECTION, SPANS, D, HEAD_DIM * N_TENSOR), D ** -0.5, 0.09375, ((0, 128), (3, 8)))
    w_key = bell_draw(keys[6], (N_SECTION, SPANS, D, HEAD_DIM), D ** -0.5, 0.09375, ((0, 128), (3, 8)))
    w_value = bell_draw(keys[7], (N_SECTION, SPANS, D, HEAD_DIM), D ** -0.5, 0.09375, ((0, 128), (3, 8)))
    return dict(acts=acts, grads_in=grads_in, head_grads=head_grads, types=types, gains=gains, w_query=w_query, w_key=w_key, w_value=w_value)


epsilon = 1e-05

def span_backward(inputs):
    x_rows, grad_rows, kind_rows, gain_pair, w_query, w_key, w_value, head_rows = inputs
    heads = w_query.shape[1] // HEAD_DIM
    groups = w_key.shape[1] // HEAD_DIM
    per_group = heads // groups
    tokens = x_rows.shape[0]
    x_float = x_rows.astype(jnp.float32)
    inverse = lax.rsqrt(lax.optimization_barrier(jnp.mean(x_float * x_float, axis=-1, keepdims=True)) + epsilon)
    gain_rows = jnp.where(kind_rows[:, None] == 1, gain_pair[1][None, :], gain_pair[0][None, :]).astype(jnp.float32)
    normed = (x_float * inverse * gain_rows).astype(jnp.bfloat16)
    queries = jnp.dot(normed, w_query, preferred_element_type=jnp.float32).astype(jnp.bfloat16).reshape(tokens, heads, HEAD_DIM)
    key_rows = jnp.dot(normed, w_key, preferred_element_type=jnp.float32).astype(jnp.bfloat16).reshape(tokens, groups, HEAD_DIM)
    value_rows = jnp.dot(normed, w_value, preferred_element_type=jnp.float32).astype(jnp.bfloat16).reshape(tokens, groups, HEAD_DIM)
    key_heads = jnp.repeat(key_rows, per_group, axis=1).astype(jnp.float32)
    value_heads = jnp.repeat(value_rows, per_group, axis=1).astype(jnp.float32)
    query_float = queries.astype(jnp.float32)
    softmax_scale = HEAD_DIM ** (-0.5)
    scores = jnp.einsum('qhd,khd->hqk', query_float, key_heads) * softmax_scale
    causal = jnp.arange(tokens)[:, None] >= jnp.arange(tokens)[None, :]
    scores = jnp.where(causal[None], scores, -1e+30)
    attn_probs = jax.nn.softmax(scores, axis=-1)
    probs_low = attn_probs.astype(jnp.bfloat16)
    out_float = head_rows.reshape(tokens, heads, HEAD_DIM).astype(jnp.float32)
    prob_grads = jnp.einsum('qhd,khd->hqk', out_float, value_heads)
    score_grads = (attn_probs * (prob_grads - lax.optimization_barrier(jnp.sum(prob_grads * attn_probs, axis=-1, keepdims=True))) * softmax_scale).astype(jnp.bfloat16)
    score_float = score_grads.astype(jnp.float32)
    query_grads = jnp.einsum('hqk,khd->qhd', score_float, key_heads).astype(jnp.bfloat16)
    key_each = jnp.einsum('hqk,qhd->khd', score_float, query_float)
    value_each = jnp.einsum('hqk,qhd->khd', probs_low.astype(jnp.float32), out_float)
    key_grads = key_each.reshape(tokens, groups, per_group, HEAD_DIM).sum(axis=2).astype(jnp.bfloat16)
    value_grads = value_each.reshape(tokens, groups, per_group, HEAD_DIM).sum(axis=2).astype(jnp.bfloat16)
    partial_value = jnp.dot(query_grads.reshape(tokens, heads * HEAD_DIM), w_query.T, preferred_element_type=jnp.float32)
    partial_value = partial_value + jnp.dot(key_grads.reshape(tokens, groups * HEAD_DIM), w_key.T, preferred_element_type=jnp.float32)
    partial_value = partial_value + jnp.dot(value_grads.reshape(tokens, groups * HEAD_DIM), w_value.T, preferred_element_type=jnp.float32)
    stat_mean = lax.optimization_barrier(jnp.mean(x_float * gain_rows * partial_value, axis=-1, keepdims=True))
    norm_grads = inverse * gain_rows * partial_value - x_float * inverse ** 3 * stat_mean
    return (grad_rows.astype(jnp.float32) + norm_grads).astype(jnp.bfloat16)

def rows_join(array):
    sections = N_SECTION // SUB
    shaped = array.reshape((sections, SUB) + array.shape[1:])
    shaped = jnp.swapaxes(shaped, 1, 2)
    return shaped.reshape((sections * SPANS, SUB * array.shape[2]) + array.shape[3:])

def cols_join(array):
    sections = N_SECTION // SUB
    shaped = array.reshape((sections, SUB) + array.shape[1:])
    shaped = jnp.moveaxis(shaped, 1, -2)
    return shaped.reshape((sections * SPANS,) + array.shape[2:-1] + (SUB * array.shape[-1],))

def reference(acts, grads_in, head_grads, types, gains, w_query, w_key, w_value):
    sections = N_SECTION // SUB
    inputs = (rows_join(acts), rows_join(grads_in), rows_join(types), cols_join(gains), cols_join(w_query), cols_join(w_key), cols_join(w_value), cols_join(head_grads))
    results = lax.map(span_backward, inputs)
    results = results.reshape(sections, SPANS, TOK, D)
    rolled = jnp.roll(results, -1, axis=0)
    rolled = rolled.at[sections - 1].set(results[0][::-1])
    shaped = rolled.reshape(sections, SPANS, SUB, TOK // SUB, D)
    shaped = jnp.swapaxes(shaped, 1, 2)
    return shaped.reshape(N_SECTION, SPANS, TOK // SUB, D)
```

```python
import jax
import jax.numpy as jnp
from jax import lax
from jax.experimental import pallas as pl
from jax.experimental.pallas import tpu as pltpu
from jax.sharding import PartitionSpec as P


HEAD_DIM = 128
SUB = 4
ROW_MASKS = (0, 2, 1, 3)

epsilon = 1e-05
F32 = jnp.float32
BF16 = jnp.bfloat16


def swapped(value, axis, mask):
    pairs = [(source, source ^ mask) for source in range(lax.axis_size(axis))]
    return lax.ppermute(value, axis, pairs)


def shifted(value, by):
    peers = lax.axis_size("section")
    return lax.ppermute(value, "section", [(i, (i + by) % peers) for i in range(peers)])


def blocks_by(value, axis, count, here, masks):
    size = value.shape[axis] // count
    return jnp.concatenate(
        [lax.dynamic_slice_in_dim(value, (here ^ m) * size, size, axis) for m in masks], axis=axis
    )


def in_quads(parts):
    tensors = lax.axis_size("tensor")
    groups = [[first + i for i in range(4)] for first in range(0, tensors, 4)]
    return lax.all_to_all(parts, "tensor", 0, 0, axis_index_groups=groups, tiled=True)


def exchanged(parts):
    return lax.all_to_all(parts, "tensor", 0, 0, tiled=True)


def copies(value, count):
    return jnp.broadcast_to(value[None], (count, *value.shape))


def norm_kernel(column, *refs):
    parts, (kind, gain, w_kv, normed, kv, inverse) = refs[:SUB], refs[SUB:]
    quads, halves, _, rows, cols = parts[0].shape
    width = quads * halves * cols
    upper = column[0] // quads
    for j, part in enumerate(parts):
        total = jnp.zeros((rows, cols), F32)
        for i in range(quads):
            for h in range(halves):
                x = part[i, h, 0].astype(F32)
                total = total + x * x
        inv = lax.rsqrt(jnp.sum(total, axis=1, keepdims=True) / width + epsilon)
        at_rows = pl.ds(j * rows, rows)
        inverse[0, at_rows, :] = inv
        speech = kind[0, at_rows, :] > 0.5
        for i in range(quads):
            for h in range(halves):
                block = (upper ^ h) * quads + i
                at = pl.ds(pl.multiple_of(block * cols, cols), cols)
                rates = jnp.where(speech, gain[0, 1:2, at], gain[0, 0:1, at])
                normed[0, at_rows, at] = (part[i, h, 0].astype(F32) * inv * rates).astype(BF16)
    kv[0] = lax.dot_general(
        w_kv[0], normed[0], (((1,), (1,)), ((), ())), preferred_element_type=F32
    ).astype(BF16)


def normalised(column, parts, kind, gain, w_kv):
    quads, halves, spans, rows, cols = parts[0].shape
    tokens = SUB * rows
    width = quads * halves * cols
    channels = w_kv.shape[1]
    x_spec = pl.BlockSpec((quads, halves, 1, rows, cols), lambda n: (0, 0, n, 0, 0))

    def whole(*shape):
        return pl.BlockSpec((1, *shape), lambda n: (n, 0, 0))

    return pl.pallas_call(
        norm_kernel,
        grid=(spans,),
        in_specs=[pl.BlockSpec(memory_space=pltpu.SMEM)]
        + [x_spec] * SUB
        + [whole(tokens, 1), whole(2, width), whole(channels, width)],
        out_specs=[whole(tokens, width), whole(channels, tokens), whole(tokens, 1)],
        out_shape=[
            jax.ShapeDtypeStruct((spans, tokens, width), BF16),
            jax.ShapeDtypeStruct((spans, channels, tokens), BF16),
            jax.ShapeDtypeStruct((spans, tokens, 1), F32),
        ],
        compiler_params=pltpu.CompilerParams(vmem_limit_bytes=16 * 1024 * 1024),
        cost_estimate=pl.CostEstimate(
            flops=2 * spans * tokens * width * (channels + 8), bytes_accessed=5_000_000, transcendentals=0
        ),
    )(column.reshape(1), *parts, kind, gain, w_kv)


def sublayers(acts, grads_in, head_grads, types, gains, w_query, w_key, w_value):
    tensors = lax.axis_size("tensor")
    sections = lax.axis_size("section") // SUB
    place = lax.axis_index("section")
    position = place % SUB
    column = lax.axis_index("tensor")
    acts, grads_in, head_grads = acts[0], grads_in[0], head_grads[0]
    spans, tokq, cols = acts.shape
    tokens = tokq * SUB
    width = cols * tensors
    quarter = gains.shape[3]

    upper = column // 4
    pair = jnp.stack([acts, swapped(acts, "tensor", 4)])
    cols_all = in_quads(copies(pair, 4))
    cols_x = swapped(cols_all, "section", 2)
    x_parts = [cols_all, cols_x, swapped(cols_all, "section", 1), swapped(cols_x, "section", 1)]

    small = jnp.concatenate(
        [
            gains[0].reshape(spans, 2 * quarter),
            jnp.pad(types[0].astype(BF16), ((0, 0), (0, 128 - tokq))),
        ],
        axis=1,
    )
    small_x = swapped(small, "section", 2)
    small_pair = jnp.stack([small, small_x])
    small_core = swapped(small_pair, "section", 1)
    small_all = jnp.concatenate([small_pair, small_core])
    kind = jnp.transpose(small_all[:, :, 2 * quarter : 2 * quarter + tokq], (1, 0, 2))
    kind = kind.reshape(spans, tokens, 1).astype(F32)
    low_bit = position & 1 == 1
    high_bit = position & 2 == 2
    rates = small_all[:, :, : 2 * quarter].reshape(2, 2, spans, 2, quarter)
    rates = jnp.where(low_bit, rates[::-1], rates)
    rates = jnp.where(high_bit, rates[:, ::-1], rates)
    gain = jnp.transpose(rates, (2, 3, 1, 0, 4)).reshape(spans, 2, width).astype(F32)

    wq = w_query[0]
    w_kv = jnp.concatenate(
        [jnp.swapaxes(w_key[0], 1, 2), jnp.swapaxes(w_value[0], 1, 2)], axis=1
    )
    part = w_kv.shape[1]
    out_grads = blocks_by(head_grads, 1, SUB, position, ROW_MASKS)

    normed, kv_part, inverse = normalised(column, x_parts, kind, gain, w_kv)

    kv_all = exchanged(copies(kv_part, tensors))
    kv_all = jnp.transpose(
        kv_all.reshape(tensors, spans, 2, part // 2, tokens), (2, 1, 0, 3, 4)
    ).reshape(2, spans, HEAD_DIM, tokens)
    key_rows, value_rows = kv_all[0], kv_all[1]

    query_float = jnp.einsum("ntd,ndh->nth", normed, wq, preferred_element_type=F32)
    queries = query_float.astype(BF16)
    scale = HEAD_DIM ** (-0.5)
    index = jnp.concatenate([(position ^ m) * tokq + jnp.arange(tokq) for m in ROW_MASKS])
    causal = index[:, None] >= index[None, :]
    scores = jnp.einsum("nqh,nhk->nqk", queries, key_rows, preferred_element_type=F32) * scale
    scores = jnp.where(causal[None], scores, -1e30)
    probs = jax.nn.softmax(scores, axis=-1)
    probs_low = probs.astype(BF16)
    prob_grads = jnp.einsum("nqh,nhk->nqk", out_grads, value_rows, preferred_element_type=F32)
    score_grads = (
        probs * (prob_grads - jnp.sum(prob_grads * probs, axis=-1, keepdims=True)) * scale
    ).astype(BF16)
    key_each = jnp.einsum("nqk,nqh->nhk", score_grads, queries, preferred_element_type=F32)
    value_each = jnp.einsum("nqk,nqh->nhk", probs_low, out_grads, preferred_element_type=F32)
    query_grads = jnp.einsum(
        "nqk,nhk->nqh", score_grads, key_rows, preferred_element_type=F32
    ).astype(BF16)
    dots = jnp.sum(query_grads.astype(F32) * query_float, axis=2)
    dots = dots + jnp.sum(
        key_each * key_rows.astype(F32) + value_each * value_rows.astype(F32), axis=1
    )
    kv_sent = jnp.concatenate(
        [
            key_each.reshape(spans, tensors, part // 2, tokens),
            value_each.reshape(spans, tensors, part // 2, tokens),
            jnp.broadcast_to(dots[:, None, None], (spans, tensors, 8, tokens)),
        ],
        axis=2,
    ).astype(BF16)
    kv_came = exchanged(jnp.transpose(kv_sent, (1, 0, 2, 3)).astype(BF16))
    kv_sum = jnp.sum(kv_came.astype(F32), axis=0)
    kv_grads = kv_sum[:, :part].astype(BF16)
    dot_sum = kv_sum[:, part]
    half = tokens // 2

    def spread(rows):
        return jnp.einsum(
            "nth,ndh->ntd", query_grads[:, rows], wq, preferred_element_type=F32
        ) + jnp.einsum("nct,ncd->ntd", kv_grads[:, :, rows], w_kv, preferred_element_type=F32)

    came = swapped(spread(slice(half, None)).astype(BF16), "section", 1)
    total = spread(slice(0, half)) + came.astype(F32)
    middle = width // 2
    halves = [lax.dynamic_slice_in_dim(total, at * middle, middle, 2) for at in (1 - upper, upper)]
    low = [rows[:, tokq:].astype(BF16) for rows in halves]
    far_came = swapped(low[0], "section", 2)
    near_came = swapped(low[1], "section", 2)

    def summed(rows, came):
        mine = (rows[:, :tokq] + came.astype(F32)).astype(BF16)
        mine = jnp.stack([mine[:, :, i * cols : (i + 1) * cols] for i in range(4)])
        return jnp.sum(in_quads(mine).astype(F32), axis=0)

    far = summed(halves[0], far_came).astype(BF16)
    far, near_came = lax.optimization_barrier((far, near_came))
    far = swapped(far, "tensor", 4)
    grad_mine = summed(halves[1], near_came) + far.astype(F32)
    dot_pair = dot_sum[:, :half] + swapped(dot_sum[:, half:], "section", 1)
    dot_mine = dot_pair[:, :tokq] + swapped(dot_pair[:, tokq:], "section", 2)
    my_inverse = inverse[:, :tokq]
    my_gain = lax.dynamic_slice_in_dim(gain, column * cols, cols, 2)
    my_gain = jnp.where(kind[:, :tokq] > 0.5, my_gain[:, 1:2], my_gain[:, 0:1])
    stat = (dot_mine / width)[..., None]
    norm_grads = my_inverse * my_gain * grad_mine - acts.astype(F32) * my_inverse**2 * stat
    result = (grads_in.astype(F32) + norm_grads).astype(BF16)
    arrived = shifted(result, -SUB)
    routed = jnp.where(place // SUB == sections - 1, arrived[::-1], arrived)
    return routed[None]


def solution(mesh):
    return jax.shard_map(
        sublayers,
        mesh=mesh,
        in_specs=(
            P("section", None, None, "tensor"),
            P("section", None, None, "tensor"),
            P("section", None, None, "tensor"),
            P("section", None, None),
            P("section", None, None, None),
            P("section", None, None, "tensor"),
            P("section", None, None, "tensor"),
            P("section", None, None, "tensor"),
        ),
        out_specs=P("section", None, None, "tensor"),
        check_vma=False,
    )
```

```python
import jax
import jax.numpy as jnp
from jax import lax
from jax.experimental import pallas as pl
from jax.experimental.pallas import tpu as pltpu
from jax.sharding import PartitionSpec as P


HEAD_DIM = 128
SUB = 4
ROW_MASKS = (0, 2, 1, 3)

epsilon = 1e-05
F32 = jnp.float32
BF16 = jnp.bfloat16


def swapped(value, axis, mask):
    pairs = [(source, source ^ mask) for source in range(lax.axis_size(axis))]
    return lax.ppermute(value, axis, pairs)


def shifted(value, by):
    peers = lax.axis_size("section")
    return lax.ppermute(value, "section", [(i, (i + by) % peers) for i in range(peers)])


def blocks_by(value, axis, count, here, masks):
    size = value.shape[axis] // count
    return jnp.concatenate(
        [lax.dynamic_slice_in_dim(value, (here ^ m) * size, size, axis) for m in masks], axis=axis
    )


def in_quads(parts):
    tensors = lax.axis_size("tensor")
    groups = [[first + i for i in range(4)] for first in range(0, tensors, 4)]
    return lax.all_to_all(parts, "tensor", 0, 0, axis_index_groups=groups, tiled=True)


def exchanged(parts):
    return lax.all_to_all(parts, "tensor", 0, 0, tiled=True)


def copies(value, count):
    return jnp.broadcast_to(value[None], (count, *value.shape))


def norm_kernel(column, *refs):
    parts, (kind, gain, w_query, w_kv, query, kv, inverse, normed) = refs[:SUB], refs[SUB:]
    quads, halves, _, rows, cols = parts[0].shape
    width = quads * halves * cols
    upper = column[0] // quads
    for j, part in enumerate(parts):
        total = jnp.zeros((rows, cols), F32)
        for i in range(quads):
            for h in range(halves):
                x = part[i, h, 0].astype(F32)
                total = total + x * x
        inv = lax.rsqrt(jnp.sum(total, axis=1, keepdims=True) / width + epsilon)
        at_rows = pl.ds(j * rows, rows)
        inverse[0, at_rows, :] = inv
        speech = kind[0, at_rows, :] > 0.5
        for i in range(quads):
            for h in range(halves):
                block = (upper ^ h) * quads + i
                at = pl.ds(pl.multiple_of(block * cols, cols), cols)
                rates = jnp.where(speech, gain[0, 1:2, at], gain[0, 0:1, at])
                normed[at_rows, at] = (part[i, h, 0].astype(F32) * inv * rates).astype(BF16)
    kv[0] = lax.dot_general(
        w_kv[0], normed[...], (((1,), (1,)), ((), ())), preferred_element_type=F32
    ).astype(BF16)
    query[0] = jnp.dot(normed[...], w_query[0], preferred_element_type=F32)


def projected(column, parts, kind, gain, w_query, w_kv):
    quads, halves, spans, rows, cols = parts[0].shape
    tokens = SUB * rows
    width = quads * halves * cols
    channels = w_kv.shape[1]
    x_spec = pl.BlockSpec((quads, halves, 1, rows, cols), lambda n: (0, 0, n, 0, 0))

    def whole(*shape):
        return pl.BlockSpec((1, *shape), lambda n: (n, 0, 0))

    return pl.pallas_call(
        norm_kernel,
        grid=(spans,),
        in_specs=[pl.BlockSpec(memory_space=pltpu.SMEM)]
        + [x_spec] * SUB
        + [whole(tokens, 1), whole(2, width), whole(width, HEAD_DIM), whole(channels, width)],
        out_specs=[whole(tokens, HEAD_DIM), whole(channels, tokens), whole(tokens, 1)],
        out_shape=[
            jax.ShapeDtypeStruct((spans, tokens, HEAD_DIM), F32),
            jax.ShapeDtypeStruct((spans, channels, tokens), BF16),
            jax.ShapeDtypeStruct((spans, tokens, 1), F32),
        ],
        scratch_shapes=[pltpu.VMEM((tokens, width), BF16)],
        compiler_params=pltpu.CompilerParams(vmem_limit_bytes=20 * 1024 * 1024),
        cost_estimate=pl.CostEstimate(
            flops=2 * spans * tokens * width * (channels + HEAD_DIM), bytes_accessed=5_000_000, transcendentals=0
        ),
    )(column.reshape(1), *parts, kind, gain, w_query, w_kv)


def sublayers(acts, grads_in, head_grads, types, gains, w_query, w_key, w_value):
    tensors = lax.axis_size("tensor")
    sections = lax.axis_size("section") // SUB
    place = lax.axis_index("section")
    position = place % SUB
    column = lax.axis_index("tensor")
    acts, grads_in, head_grads = acts[0], grads_in[0], head_grads[0]
    spans, tokq, cols = acts.shape
    tokens = tokq * SUB
    width = cols * tensors
    quarter = gains.shape[3]

    upper = column // 4
    across = swapped(acts, "tensor", 4)
    shape = (4, 1, *acts.shape)
    cols_all = jnp.concatenate(
        [jnp.broadcast_to(acts, shape), jnp.broadcast_to(across, shape)], axis=1
    )
    cols_all = in_quads(cols_all)
    cols_x = swapped(cols_all, "section", 2)
    x_parts = [cols_all, cols_x, swapped(cols_all, "section", 1), swapped(cols_x, "section", 1)]

    small = jnp.concatenate(
        [
            gains[0].reshape(spans, 2 * quarter),
            jnp.pad(types[0].astype(BF16), ((0, 0), (0, 128 - tokq))),
        ],
        axis=1,
    )
    small_x = swapped(small, "section", 2)
    small_pair = jnp.stack([small, small_x])
    small_core = swapped(small_pair, "section", 1)
    small_all = jnp.concatenate([small_pair, small_core])
    kind = jnp.transpose(small_all[:, :, 2 * quarter : 2 * quarter + tokq], (1, 0, 2))
    kind = kind.reshape(spans, tokens, 1).astype(F32)
    low_bit = position & 1 == 1
    high_bit = position & 2 == 2
    rates = small_all[:, :, : 2 * quarter].reshape(2, 2, spans, 2, quarter)
    rates = jnp.where(low_bit, rates[::-1], rates)
    rates = jnp.where(high_bit, rates[:, ::-1], rates)
    gain = jnp.transpose(rates, (2, 3, 1, 0, 4)).reshape(spans, 2, width).astype(F32)

    wq = w_query[0]
    w_kv = jnp.concatenate(
        [jnp.swapaxes(w_key[0], 1, 2), jnp.swapaxes(w_value[0], 1, 2)], axis=1
    )
    part = w_kv.shape[1]
    out_grads = blocks_by(head_grads, 1, SUB, position, ROW_MASKS)

    query_float, kv_part, inverse = projected(column, x_parts, kind, gain, wq, w_kv)

    kv_all = exchanged(copies(kv_part, tensors))
    kv_all = jnp.transpose(
        kv_all.reshape(tensors, spans, 2, part // 2, tokens), (2, 1, 0, 3, 4)
    ).reshape(2, spans, HEAD_DIM, tokens)
    key_rows, value_rows = kv_all[0], kv_all[1]

    queries = query_float.astype(BF16)
    scale = HEAD_DIM ** (-0.5)
    index = jnp.concatenate([(position ^ m) * tokq + jnp.arange(tokq) for m in ROW_MASKS])
    causal = index[:, None] >= index[None, :]
    scores = jnp.einsum("nqh,nhk->nqk", queries, key_rows, preferred_element_type=F32) * scale
    scores = jnp.where(causal[None], scores, -1e30)
    probs = jax.nn.softmax(scores, axis=-1)
    probs_low = probs.astype(BF16)
    prob_grads = jnp.einsum("nqh,nhk->nqk", out_grads, value_rows, preferred_element_type=F32)
    score_grads = (
        probs * (prob_grads - jnp.sum(prob_grads * probs, axis=-1, keepdims=True)) * scale
    ).astype(BF16)
    key_each = jnp.einsum("nqk,nqh->nhk", score_grads, queries, preferred_element_type=F32)
    value_each = jnp.einsum("nqk,nqh->nhk", probs_low, out_grads, preferred_element_type=F32)
    query_grads = jnp.einsum(
        "nqk,nhk->nqh", score_grads, key_rows, preferred_element_type=F32
    ).astype(BF16)
    dots = jnp.sum(query_grads.astype(F32) * query_float, axis=2)
    dots = dots + jnp.sum(
        key_each * key_rows.astype(F32) + value_each * value_rows.astype(F32), axis=1
    )
    kv_sent = jnp.concatenate(
        [
            key_each.reshape(spans, tensors, part // 2, tokens),
            value_each.reshape(spans, tensors, part // 2, tokens),
            jnp.broadcast_to(dots[:, None, None], (spans, tensors, 8, tokens)),
        ],
        axis=2,
    ).astype(BF16)
    kv_came = exchanged(jnp.transpose(kv_sent, (1, 0, 2, 3)).astype(BF16))
    kv_sum = jnp.sum(kv_came.astype(F32), axis=0)
    kv_grads = kv_sum[:, :part].astype(BF16)
    dot_sum = kv_sum[:, part]
    half = tokens // 2

    def spread(rows):
        return jnp.einsum(
            "nth,ndh->ntd", query_grads[:, rows], wq, preferred_element_type=F32
        ) + jnp.einsum("nct,ncd->ntd", kv_grads[:, :, rows], w_kv, preferred_element_type=F32)

    came = swapped(spread(slice(half, None)).astype(BF16), "section", 1)
    total = spread(slice(0, half)) + came.astype(F32)
    middle = width // 2
    halves = [lax.dynamic_slice_in_dim(total, at * middle, middle, 2) for at in (1 - upper, upper)]
    low = [rows[:, tokq:].astype(BF16) for rows in halves]
    far_came = swapped(low[0], "section", 2)
    near_came = swapped(low[1], "section", 2)

    def summed(rows, came):
        mine = (rows[:, :tokq] + came.astype(F32)).astype(BF16)
        mine = jnp.stack([mine[:, :, i * cols : (i + 1) * cols] for i in range(4)])
        return jnp.sum(in_quads(mine).astype(F32), axis=0)

    far = summed(halves[0], far_came).astype(BF16)
    far, near_came = lax.optimization_barrier((far, near_came))
    far = swapped(far, "tensor", 4)
    grad_mine = summed(halves[1], near_came) + far.astype(F32)
    dot_pair = dot_sum[:, :half] + swapped(dot_sum[:, half:], "section", 1)
    dot_mine = dot_pair[:, :tokq] + swapped(dot_pair[:, tokq:], "section", 2)
    my_inverse = inverse[:, :tokq]
    my_gain = lax.dynamic_slice_in_dim(gain, column * cols, cols, 2)
    my_gain = jnp.where(kind[:, :tokq] > 0.5, my_gain[:, 1:2], my_gain[:, 0:1])
    stat = (dot_mine / width)[..., None]
    norm_grads = my_inverse * my_gain * grad_mine - acts.astype(F32) * my_inverse**2 * stat
    result = (grads_in.astype(F32) + norm_grads).astype(BF16)
    arrived = shifted(result, -SUB)
    routed = jnp.where(place // SUB == sections - 1, arrived[::-1], arrived)
    return routed[None]


def solution(mesh):
    return jax.shard_map(
        sublayers,
        mesh=mesh,
        in_specs=(
            P("section", None, None, "tensor"),
            P("section", None, None, "tensor"),
            P("section", None, None, "tensor"),
            P("section", None, None),
            P("section", None, None, None),
            P("section", None, None, "tensor"),
            P("section", None, None, "tensor"),
            P("section", None, None, "tensor"),
        ),
        out_specs=P("section", None, None, "tensor"),
        check_vma=False,
    )
```
